32 devices in a mesh: grp: 8 (over z, x), sub: 4 (over y, core).
Axes of the slice: x: 2, y: 2, z: 4, core: 2. Of those that a mesh axis runs over, the one named last changes fastest.
Arguments:
- residual: float32 [98304], P(('grp', 'sub')), may hold values from -6 to 6
- edge_scale: float32 [98304], P(('grp', 'sub')), may hold values from 0.2 to 1
- tangent: float32 [3, 98304], P(None, ('grp', 'sub')), may hold values from -6 to 6
- edge_tail: int32 [98304], P(('grp', 'sub')), may hold values from 0 to 511
- edge_head: int32 [98304], P(('grp', 'sub')), may hold values from 0 to 4607
- stencil_index: int32 [14, 16384], P(None, ('grp', 'sub')), may hold values from 0 to 4607
- stencil_coef: bfloat16 [4, 14, 16384], P(None, None, ('grp', 'sub')), may hold values from -1 to -0.099609375
- diag_margin: float32 [4, 16384], P(None, ('grp', 'sub')), may hold values from 0.05 to 0.5
- send_index: int32 [16, 8, 512], P('grp', 'sub'), may hold values from 0 to 511
Outputs:
- correction: float32 [98304], P(('grp', 'sub'))
The draws below stay inside these ranges and needn't reach their ends.
Inputs may be any that keep to these rules, and one draw needn't show every extreme that they name: `edge_tail`: positions among a device's own nodes. `edge_head`: positions in the device's extended list: own nodes first, then the 8 received blocks. `stencil_index`: positions in the extended list of the device that holds the row. `send_index`: positions among the device's own nodes; an entry may repeat.
All inputs are finite; a program needn't handle non-finite values.
Results may differ from the reference program's by a relative error of at most 0.0003.
Values sent between devices are 32-bit elements; how exact they have to be, the bound alone decides.
A program may use at most 64 MiB of HBM per device.

```python
import math
import jax
import jax.numpy as jnp

N_DEV = 512
E_DEV = 3072
HALO = 512
STENCIL = 14
SWEEPS = 4
NODES = 16384
EDGES = 98304
N_GRP = 8
N_SUB = 4


def with_ends(entries, stream_key, smallest, top_value):
    longest = entries.shape.index(max(entries.shape))
    spots = []
    for shift in (0, 1):
        where = [jax.random.randint(jax.random.fold_in(stream_key, axis), (), 0, length) for axis, length in enumerate(entries.shape)]
        where[longest] = (where[longest] + shift) % entries.shape[longest]
        spots.append(tuple(where))
    return entries.at[spots[0]].set(smallest).at[spots[1]].set(top_value)


def steps_of(stream_key, extent, pieces, smallest, largest):
    factor_of, own = 1.0, jax.random.fold_in(stream_key, 6)
    for dim, shards_of in pieces:
        draws = jnp.exp(jax.random.uniform(jax.random.fold_in(own, dim), (shards_of,), jnp.float32, smallest / len(pieces), largest / len(pieces)))
        factor_of = factor_of * jnp.repeat(draws, extent[dim] // shards_of).reshape([-1 if axis == dim else 1 for axis in range(len(extent))])
    return factor_of


def scatter_about(key, shape, scale, bound, cuts=(), kind=jnp.bfloat16):
    drawn = jax.random.normal(key, shape, jnp.float32) * scale
    if len(cuts) > 0:
        drawn = steps_of(key, shape, cuts, -0.22, 0.18) * drawn
    return jnp.clip(drawn, min=-bound, max=bound).astype(kind)


def setup_inputs(seed: int = 0) -> dict:
    arg_keys = jax.random.split(jax.random.key(seed), 10)
    return {
        "residual": scatter_about(arg_keys[0], (EDGES,), 1.0, 6.0, ((0, 32),), jnp.float32),
        "edge_scale": jnp.clip(jnp.exp(math.log(1.0) - 1.609438 * jax.random.uniform(arg_keys[1], (EDGES,), jnp.float32) ** steps_of(arg_keys[1], (EDGES,), ((0, 32),), -0.2, 0.2)), 0.2, 1.0),
        "tangent": scatter_about(arg_keys[2], (3, EDGES), 1.0, 6.0, ((1, 32),), jnp.float32),
        "edge_tail": with_ends(jax.random.randint(arg_keys[3], (EDGES,), 0, N_DEV), jax.random.fold_in(arg_keys[3], 1), 0, N_DEV - 1).astype(jnp.int32),
        "edge_head": with_ends(jax.random.randint(arg_keys[4], (EDGES,), 0, N_DEV + 8 * HALO), jax.random.fold_in(arg_keys[4], 1), 0, (N_DEV + 8 * HALO) - 1).astype(jnp.int32),
        "stencil_index": with_ends(jax.random.randint(arg_keys[5], (STENCIL, NODES), 0, N_DEV + 8 * HALO), jax.random.fold_in(arg_keys[5], 1), 0, (N_DEV + 8 * HALO) - 1).astype(jnp.int32),
        "stencil_coef": jnp.clip(-1.0 + 0.9003906 * jax.random.uniform(arg_keys[6], (4, STENCIL, NODES), jnp.float32) ** steps_of(arg_keys[6], (4, STENCIL, NODES), ((2, 32),), -0.2, 0.2), -1.0, -0.099609375).astype(jnp.bfloat16),
        "diag_margin": jnp.clip(jnp.exp(math.log(0.5) - 2.3025851 * jax.random.uniform(arg_keys[7], (4, NODES), jnp.float32) ** steps_of(arg_keys[7], (4, NODES), ((1, 32),), -0.2, 0.2)), 0.05, 0.5),
        "send_index": with_ends(jax.random.randint(arg_keys[8], (2 * N_GRP, 2 * N_SUB, HALO), 0, N_DEV), jax.random.fold_in(arg_keys[8], 1), 0, N_DEV - 1).astype(jnp.int32),
    }


def ghost_table(send_index):
    blocks = send_index.reshape(N_GRP, 2, N_SUB, 2, HALO).transpose(0, 2, 1, 3, 4)
    owner_base = (jnp.arange(N_GRP * N_SUB, dtype=jnp.int32) * N_DEV).reshape(N_GRP, N_SUB, 1, 1, 1)
    global_ids = blocks + owner_base
    from_below = jnp.roll(global_ids, 1, axis=0)[:, :, 1]
    from_above = jnp.roll(global_ids, -1, axis=0)[:, :, 0]
    from_prev = jnp.roll(global_ids, 1, axis=1)[:, :, :, 1]
    from_next = jnp.roll(global_ids, -1, axis=1)[:, :, :, 0]
    ghosts = jnp.concatenate([from_below, from_above, from_prev, from_next], axis=2)
    ghosts = ghosts.reshape(N_GRP * N_SUB, 8 * HALO)
    own_ids = jnp.arange(N_GRP * N_SUB * N_DEV, dtype=jnp.int32).reshape(N_GRP * N_SUB, N_DEV)
    return jnp.concatenate([own_ids, ghosts], axis=1).reshape(-1)


def to_global(flat_table, local, per_device):
    extended = N_DEV + 8 * HALO
    device = (jnp.arange(local.shape[-1], dtype=jnp.int32) // per_device).astype(jnp.int32)
    return flat_table[device * extended + local.astype(jnp.int32)]


def reference(residual, edge_scale, tangent, edge_tail, edge_head, stencil_index, stencil_coef, diag_margin, send_index):
    flat_table = ghost_table(send_index)
    tail_ids = to_global(flat_table, edge_tail, E_DEV)
    head_ids = to_global(flat_table, edge_head, E_DEV)
    node_total = N_DEV * N_GRP * N_SUB
    half_terms = 0.5 * tangent * residual[None, :]
    vals_tail = jnp.concatenate([-residual[None, :], half_terms], axis=0)
    vals_head = jnp.concatenate([residual[None, :], half_terms], axis=0)
    node_sums = jnp.zeros((4, node_total), jnp.float32)
    node_sums = node_sums.at[:, tail_ids].add(vals_tail).at[:, head_ids].add(vals_head)
    neighbour_ids = [to_global(flat_table, stencil_index[column], N_DEV) for column in range(STENCIL)]
    diag_vals = jnp.zeros((4, node_total), jnp.float32)
    for column in range(STENCIL):
        diag_vals = diag_vals + jnp.abs(stencil_coef[:, column].astype(jnp.float32))
    diag_vals = (1.0 + diag_margin) * diag_vals
    solved = node_sums / diag_vals
    for sweep in range(SWEEPS - 1):
        applied = diag_vals * solved
        for column in range(STENCIL):
            applied = applied + stencil_coef[:, column].astype(jnp.float32) * solved[:, neighbour_ids[column]]
        solved = solved + (node_sums - applied) / diag_vals
    at_tail = solved[:, tail_ids]
    at_head = solved[:, head_ids]
    return edge_scale * residual + (at_head[0] - at_tail[0]) + 0.5 * jnp.sum(tangent * (at_tail[1:] + at_head[1:]), axis=0)
```

```python
import functools

import jax
import jax.numpy as jnp
from jax import lax
from jax.experimental import pallas as pl
from jax.experimental.pallas import tpu as pltpu
from jax.sharding import PartitionSpec as P

SWEEPS = 4
LANES = 128
OPP = (0, 2, 1, 4, 3)
MESH = pl.DeviceIdType.MESH
DNUMS = lax.GatherDimensionNumbers(
    offset_dims=(),
    collapsed_slice_dims=(1,),
    start_index_map=(1,),
    operand_batching_dims=(0,),
    start_indices_batching_dims=(0,),
)
F32 = jnp.float32
BF16 = jnp.bfloat16


def lane_gather(table, lane):
    return lax.gather(
        table,
        lane[..., None],
        DNUMS,
        slice_sizes=(1, 1),
        mode=lax.GatherScatterMode.PROMISE_IN_BOUNDS,
    )


def nt_dot(a, b):
    return lax.dot_general(a, b, (((1,), (1,)), ((), ())), preferred_element_type=F32)


def kernel(
    res_h, tan_h, tail_h, head_h, sidx_h, coef_h, marg_h, send_h,
    out_ref,
    res, tan, tail, head, sidx, coef, marg, own_send,
    got_send, psend, got_p, tab, onehot, spread, onehot2, spread2,
    cf, bsc, diag, hq, hl, sq, sl, tan2,
    local_sem, send_sem, recv_sem,
):
    G, S = lax.axis_size("grp"), lax.axis_size("sub")
    g, s = lax.axis_index("grp"), lax.axis_index("sub")
    gm, gp = lax.rem(g + G - 1, G), lax.rem(g + 1, G)
    sm, sp = lax.rem(s + S - 1, S), lax.rem(s + 1, S)
    peer = (None, (gm, s), (gp, s), (g, sm), (g, sp))
    order = (4, 3, 2, 1)
    nrow = marg.shape[1] // LANES
    erow = res.shape[0]
    stencil = sidx.shape[0]
    vrow = 4 * nrow
    nq = 5 * nrow
    hrow = got_send.shape[3] // LANES

    barrier = pltpu.get_barrier_semaphore()
    for o in order:
        pl.semaphore_signal(barrier, inc=1, device_id=peer[o], device_id_type=MESH)
    pairs = (
        (tail_h, tail), (res_h, res), (tan_h, tan), (head_h, head),
        (coef_h, coef), (marg_h, marg), (sidx_h, sidx),
    )
    local = [
        pltpu.make_async_copy(src, dst, local_sem.at[i]) for i, (src, dst) in enumerate(pairs)
    ]
    for c in local:
        c.start()

    def exchange(rnd, src, dst):
        copies = {}
        for o in order:
            copies[o] = pltpu.make_async_remote_copy(
                src_ref=src(o),
                dst_ref=dst(OPP[o]),
                send_sem=send_sem.at[rnd, o - 1],
                recv_sem=recv_sem.at[rnd, OPP[o] - 1],
                device_id=peer[o],
                device_id_type=MESH,
            )
            copies[o].start()
        return copies

    def arrived(copies, o):
        copies[OPP[o]].wait_recv()

    pl.semaphore_wait(barrier, 4)
    rounds = [exchange(0, lambda o: send_h, lambda o: got_send.at[o - 1])]

    for c in local:
        c.wait()
    riota = lax.broadcasted_iota(jnp.int32, (vrow, LANES), 0)
    kind = riota // nrow
    rpart = riota - kind * nrow
    liota = lax.broadcasted_iota(jnp.int32, (LANES, LANES), 0)

    def terms(t, sign):
        r = res[t : t + 1, :]
        first = jnp.broadcast_to(r if sign > 0 else -r, (vrow, LANES))
        half = 0.5 * r
        val = first
        for c in range(3):
            v = tan[c : c + 1, t * LANES : (t + 1) * LANES] * half
            val = jnp.where(kind == c + 1, v, val)
        hi = val.astype(BF16).astype(F32)
        return hi, val - hi

    def scatter(spread_ref, onehot_ref, lanes_of, rows_of, owners, sign):
        for t in range(erow):
            cols = slice(t * LANES, (t + 1) * LANES)
            onehot_ref[:, cols] = jnp.where(liota == lanes_of(t), 1.0, 0.0).astype(BF16)
            hi, lo = terms(t, sign)
            row = rows_of(t)
            for o in range(owners):
                hit = row == rpart + o * nrow
                for p, v in enumerate((hi, lo)):
                    base = (p * owners + o) * vrow
                    spread_ref[base : base + vrow, cols] = jnp.where(hit, v, 0.0).astype(BF16)
        both = nt_dot(spread_ref[...], onehot_ref[...])
        return both[: owners * vrow] + both[owners * vrow :]

    own_sum = scatter(
        spread, onehot,
        lambda t: tail[t : t + 1, :] & (LANES - 1),
        lambda t: tail[t : t + 1, :] >> 7,
        1, -1,
    )

    cf[...] = jnp.zeros_like(cf)
    for k in range(4):
        for r in range(nrow):
            cols = slice(r * LANES, (r + 1) * LANES)
            c = coef[k, :, cols].astype(F32)
            d = (1.0 + marg[k : k + 1, cols]) * jnp.sum(jnp.abs(c), axis=0, keepdims=True)
            inv = 1.0 / d
            diag[k * nrow + r : k * nrow + r + 1, :] = inv
            cf[k, :stencil, cols] = c * inv
    for c in range(3):
        for t in range(erow):
            tan2[c * erow + t : c * erow + t + 1, :] = tan[c : c + 1, t * LANES : (t + 1) * LANES]
    sq[...] = jnp.zeros_like(sq)
    sq[:stencil, :] = sidx[...]

    for o in order:
        arrived(rounds[0], o)
    halves = (
        None,
        ((1, 0), (1, 1)),
        ((0, 0), (0, 1)),
        ((0, 1), (1, 1)),
        ((0, 0), (1, 0)),
    )

    def compose(x):
        lane = x & (LANES - 1)
        row = x >> 7
        y = x
        at = nrow
        for o in range(1, 5):
            for a, b in halves[o]:
                for r in range(hrow):
                    line = got_send[o - 1, a, b : b + 1, r * LANES : (r + 1) * LANES]
                    line = jnp.broadcast_to(line + o * nrow * LANES, x.shape)
                    y = jnp.where(row == at, lane_gather(line, lane), y)
                    at += 1
        return y

    for i in range(erow // 8):
        y = compose(head[i * 8 : i * 8 + 8, :])
        hq[i * 8 : i * 8 + 8, :] = y >> 7
        hl[i * 8 : i * 8 + 8, :] = y & (LANES - 1)

    parts = scatter(
        spread2, onehot2,
        lambda t: hl[t : t + 1, :],
        lambda t: hq[t : t + 1, :],
        5, 1,
    )
    psend[...] = parts[vrow:]
    own_sum = own_sum + parts[:vrow]
    rounds.append(
        exchange(
            1,
            lambda o: psend.at[pl.ds((o - 1) * vrow, vrow)],
            lambda o: got_p.at[pl.ds((o - 1) * vrow, vrow)],
        )
    )

    srows = sq.shape[0] // 8
    for i in range(srows):
        for r in range(nrow):
            cols = slice(r * LANES, (r + 1) * LANES)
            y = compose(sq[i * 8 : i * 8 + 8, cols])
            sq[i * 8 : i * 8 + 8, cols] = y >> 7
            sl[i * 8 : i * 8 + 8, cols] = y & (LANES - 1)

    for o in order:
        arrived(rounds[1], o)
        own_sum = own_sum + got_p[(o - 1) * vrow : o * vrow, :]
    bsc[...] = own_sum * diag[...]

    def look(rnd, o, r, k, shape):
        at = o * vrow + k * nrow + r
        return jnp.broadcast_to(tab[rnd, at : at + 1, :], shape)

    def add_rows(rnd, o, rows, lanes, accs):
        for r in range(nrow):
            for i in range(len(rows)):
                hit = rows[i] == o * nrow + r
                for k in range(4):
                    v = lane_gather(look(rnd, o, r, k, rows[i].shape), lanes[i])
                    accs[i][k] = v if accs[i][k] is None else jnp.where(hit, v, accs[i][k])

    for rnd in range(SWEEPS):
        if rnd == 0:
            tab[rnd, :vrow, :] = bsc[...]
        copies = exchange(
            2 + rnd,
            lambda o: tab.at[rnd, pl.ds(0, vrow)],
            lambda o: tab.at[rnd, pl.ds(o * vrow, vrow)],
        )
        rounds.append(copies)
        if rnd < SWEEPS - 1:
            where = [(slice(i * 8, i * 8 + 8), slice(r * LANES, (r + 1) * LANES)) for i in range(srows) for r in range(nrow)]
            rows = [sq[w] for w in where]
            lanes = [sl[w] for w in where]
            accs = [[None] * 4 for _ in where]
            add_rows(rnd, 0, rows, lanes, accs)
            for o in order:
                arrived(copies, o)
                add_rows(rnd, o, rows, lanes, accs)
            for k in range(4):
                for r in range(nrow):
                    total = None
                    for i in range(srows):
                        n = i * nrow + r
                        v = accs[n][k] * cf[(k,) + where[n]]
                        total = v if total is None else total + v
                    at = k * nrow + r
                    tab[rnd + 1, at : at + 1, :] = bsc[at : at + 1, :] - jnp.sum(total, axis=0, keepdims=True)

    last = SWEEPS - 1
    n3 = erow // 8
    where = [slice(i * 8, i * 8 + 8) for i in range(n3)]
    tails = [tail[w, :] for w in where]
    tacc = [[None] * 4 for _ in where]
    add_rows(last, 0, [t >> 7 for t in tails], [t & (LANES - 1) for t in tails], tacc)
    rows = [hq[w, :] for w in where]
    lanes = [hl[w, :] for w in where]
    hacc = [[None] * 4 for _ in where]
    add_rows(last, 0, rows, lanes, hacc)
    for o in order:
        arrived(copies, o)
        add_rows(last, o, rows, lanes, hacc)
    for i, w in enumerate(where):
        mixed = None
        for c in range(3):
            v = tan2[c * erow + i * 8 : c * erow + i * 8 + 8, :] * (tacc[i][c + 1] + hacc[i][c + 1])
            mixed = v if mixed is None else mixed + v
        out_ref[w, :] = (hacc[i][0] - tacc[i][0]) + 0.5 * mixed

    for copies in rounds:
        for o in order:
            copies[o].wait_send()


def body(
    residual, edge_scale, tangent, edge_tail, edge_head,
    stencil_index, stencil_coef, diag_margin, send_index,
):
    edges = residual.shape[0]
    erow = edges // LANES
    nodes = diag_margin.shape[1]
    nrow = nodes // LANES
    vrow = 4 * nrow
    stencil = stencil_index.shape[0]
    spad = -(-stencil // 8) * 8
    square = lambda x: x.reshape(erow, LANES)
    anyspace = pl.BlockSpec(memory_space=pl.ANY)
    vm = pltpu.VMEM
    i32 = jnp.int32
    gathered = pl.pallas_call(
        kernel,
        out_shape=jax.ShapeDtypeStruct((erow, LANES), F32),
        in_specs=[anyspace] * 8,
        out_specs=pl.BlockSpec(memory_space=vm),
        scratch_shapes=[
            vm((erow, LANES), F32),
            vm(tangent.shape, F32),
            vm((erow, LANES), i32),
            vm((erow, LANES), i32),
            vm(stencil_index.shape, i32),
            vm(stencil_coef.shape, BF16),
            vm(diag_margin.shape, F32),
            vm(send_index.shape, i32),
            vm((4,) + send_index.shape, i32),
            vm((4 * vrow, LANES), F32),
            vm((4 * vrow, LANES), F32),
            vm((SWEEPS, 5 * vrow, LANES), F32),
            vm((LANES, edges), BF16),
            vm((2 * vrow, edges), BF16),
            vm((LANES, edges), BF16),
            vm((10 * vrow, edges), BF16),
            vm((4, spad, nodes), F32),
            vm((vrow, LANES), F32),
            vm((vrow, LANES), F32),
            vm((erow, LANES), i32),
            vm((erow, LANES), i32),
            vm((spad, nodes), i32),
            vm((spad, nodes), i32),
            vm((3 * erow, LANES), F32),
            pltpu.SemaphoreType.DMA((7,)),
            pltpu.SemaphoreType.DMA((SWEEPS + 2, 4)),
            pltpu.SemaphoreType.DMA((SWEEPS + 2, 4)),
        ],
        compiler_params=pltpu.CompilerParams(collective_id=0, has_side_effects=True),
    )(
        square(residual), tangent, square(edge_tail), square(edge_head),
        stencil_index, stencil_coef, diag_margin, send_index,
    )
    return edge_scale * residual + gathered.reshape(edges)


def solution(mesh):
    return jax.shard_map(
        body,
        mesh=mesh,
        in_specs=(
            P(("grp", "sub")),
            P(("grp", "sub")),
            P(None, ("grp", "sub")),
            P(("grp", "sub")),
            P(("grp", "sub")),
            P(None, ("grp", "sub")),
            P(None, None, ("grp", "sub")),
            P(None, ("grp", "sub")),
            P("grp", "sub", None),
        ),
        out_specs=P(("grp", "sub")),
        check_vma=False,
    )
```

```python
import functools

import jax
import jax.numpy as jnp
from jax import lax
from jax.experimental import pallas as pl
from jax.experimental.pallas import tpu as pltpu
from jax.sharding import PartitionSpec as P

SWEEPS = 4
LANES = 128
OPP = (0, 2, 1, 4, 3)
MESH = pl.DeviceIdType.MESH
DNUMS = lax.GatherDimensionNumbers(
    offset_dims=(),
    collapsed_slice_dims=(1,),
    start_index_map=(1,),
    operand_batching_dims=(0,),
    start_indices_batching_dims=(0,),
)
F32 = jnp.float32
BF16 = jnp.bfloat16


def lane_gather(table, lane):
    return lax.gather(
        table,
        lane[..., None],
        DNUMS,
        slice_sizes=(1, 1),
        mode=lax.GatherScatterMode.PROMISE_IN_BOUNDS,
    )


def nt_dot(a, b):
    return lax.dot_general(a, b, (((1,), (1,)), ((), ())), preferred_element_type=F32)


def kernel(
    res_h, tan_h, tail_h, head_h, sidx_h, coef_h, marg_h, send_h,
    out_ref,
    res, tan, tail, head, sidx, coef, marg, own_send,
    got_send, psend, got_p, tab, onehot, spread, onehot2, spread2, onehot3, spread3, tsum,
    cf, bsc, diag, hq, hl, sq, sl, tan2,
    local_sem, send_sem, recv_sem,
):
    G, S = lax.axis_size("grp"), lax.axis_size("sub")
    g, s = lax.axis_index("grp"), lax.axis_index("sub")
    gm, gp = lax.rem(g + G - 1, G), lax.rem(g + 1, G)
    sm, sp = lax.rem(s + S - 1, S), lax.rem(s + 1, S)
    peer = (None, (gm, s), (gp, s), (g, sm), (g, sp))
    order = (4, 3, 2, 1)
    nrow = marg.shape[1] // LANES
    erow = res.shape[0]
    stencil = sidx.shape[0]
    vrow = 4 * nrow
    nq = 5 * nrow
    hrow = got_send.shape[3] // LANES

    barrier = pltpu.get_barrier_semaphore()
    for o in order:
        pl.semaphore_signal(barrier, inc=1, device_id=peer[o], device_id_type=MESH)
    pairs = (
        (tail_h, tail), (res_h, res), (tan_h, tan), (head_h, head),
        (send_h, own_send), (coef_h, coef), (marg_h, marg), (sidx_h, sidx),
    )
    local = [
        pltpu.make_async_copy(src, dst, local_sem.at[i]) for i, (src, dst) in enumerate(pairs)
    ]
    for c in local:
        c.start()

    def exchange(rnd, src, dst):
        copies = {}
        for o in order:
            copies[o] = pltpu.make_async_remote_copy(
                src_ref=src(o),
                dst_ref=dst(OPP[o]),
                send_sem=send_sem.at[rnd, o - 1],
                recv_sem=recv_sem.at[rnd, OPP[o] - 1],
                device_id=peer[o],
                device_id_type=MESH,
            )
            copies[o].start()
        return copies

    def arrived(copies, o):
        copies[OPP[o]].wait_recv()

    for c in local:
        c.wait()
    riota = lax.broadcasted_iota(jnp.int32, (vrow, LANES), 0)
    kind = riota // nrow
    rpart = riota - kind * nrow
    liota = lax.broadcasted_iota(jnp.int32, (LANES, LANES), 0)

    def terms(t, sign):
        r = res[t : t + 1, :]
        first = jnp.broadcast_to(r if sign > 0 else -r, (vrow, LANES))
        half = 0.5 * r
        val = first
        for c in range(3):
            v = tan[c : c + 1, t * LANES : (t + 1) * LANES] * half
            val = jnp.where(kind == c + 1, v, val)
        hi = val.astype(BF16).astype(F32)
        return hi, val - hi

    def scatter(spread_ref, onehot_ref, lanes_of, rows_of, owners, sign):
        for t in range(erow):
            cols = slice(t * LANES, (t + 1) * LANES)
            onehot_ref[:, cols] = jnp.where(liota == lanes_of(t), 1.0, 0.0).astype(BF16)
            hi, lo = terms(t, sign)
            row = rows_of(t)
            for o in range(owners):
                hit = row == rpart + o * nrow
                for p, v in enumerate((hi, lo)):
                    base = (p * owners + o) * vrow
                    spread_ref[base : base + vrow, cols] = jnp.where(hit, v, 0.0).astype(BF16)
        both = nt_dot(spread_ref[...], onehot_ref[...])
        return both[: owners * vrow] + both[owners * vrow :]

    own_sum = scatter(
        spread, onehot,
        lambda t: tail[t : t + 1, :] & (LANES - 1),
        lambda t: tail[t : t + 1, :] >> 7,
        1, -1,
    )

    parts = scatter(
        spread2, onehot2,
        lambda t: head[t : t + 1, :] & (LANES - 1),
        lambda t: head[t : t + 1, :] >> 7,
        (nrow + 8 * hrow) // nrow, 1,
    )
    psend[...] = parts[vrow:]
    own_sum = own_sum + parts[:vrow]
    sent = 2 * 4 * hrow

    lists = tuple((a, b, r) for a in range(2) for b in range(2) for r in range(hrow))

    def own_list(a, b, r):
        return own_send[a, b : b + 1, r * LANES : (r + 1) * LANES]

    for n, abr in enumerate(lists):
        hit = liota == (own_list(*abr) & (LANES - 1))
        onehot3[:, n * LANES : (n + 1) * LANES] = jnp.where(hit, 1.0, 0.0).astype(BF16)

    cf[...] = jnp.zeros_like(cf)
    for k in range(4):
        for r in range(nrow):
            cols = slice(r * LANES, (r + 1) * LANES)
            c = coef[:, k, cols].astype(F32)
            d = (1.0 + marg[k : k + 1, cols]) * jnp.sum(jnp.abs(c), axis=0, keepdims=True)
            inv = 1.0 / d
            diag[k * nrow + r : k * nrow + r + 1, :] = inv
            cf[k, :stencil, cols] = c * inv
    for c in range(3):
        for t in range(erow):
            tan2[c * erow + t : c * erow + t + 1, :] = tan[c : c + 1, t * LANES : (t + 1) * LANES]
    sq[...] = jnp.zeros_like(sq)
    sq[:stencil, :] = sidx[...]

    pl.semaphore_wait(barrier, 4)
    rounds = [
        exchange(
            1,
            lambda o: psend.at[pl.ds((o - 1) * sent, sent)],
            lambda o: got_p.at[pl.ds((o - 1) * sent, sent)],
        )
    ]
    rounds.append(exchange(0, lambda o: own_send, lambda o: got_send.at[o - 1]))

    for o in order:
        arrived(rounds[0], o)
    block = 4 * hrow
    for a in range(2):
        for b in range(2):
            first = a * sent + b * block
            second = (2 + b) * sent + a * block
            at = (a * 2 + b) * block
            tsum[at : at + block, :] = got_p[first : first + block, :] + got_p[second : second + block, :]
    for n, (a, b, r) in enumerate(lists):
        base = (a * 2 + b) * block + r
        val = jnp.broadcast_to(tsum[base : base + 1, :], (vrow, LANES))
        for k in range(1, 4):
            at = base + k * hrow
            val = jnp.where(kind == k, tsum[at : at + 1, :], val)
        hit = (own_list(a, b, r) >> 7) == rpart
        val = jnp.where(hit, val, 0.0)
        hi = val.astype(BF16)
        cols = slice(n * LANES, (n + 1) * LANES)
        spread3[:vrow, cols] = hi
        spread3[vrow:, cols] = (val - hi.astype(F32)).astype(BF16)
    back = nt_dot(spread3[...], onehot3[...])
    own_sum = own_sum + (back[:vrow] + back[vrow:])
    bsc[...] = own_sum * diag[...]

    halves = (
        None,
        ((1, 0), (1, 1)),
        ((0, 0), (0, 1)),
        ((0, 1), (1, 1)),
        ((0, 0), (1, 0)),
    )

    def compose(x):
        lane = x & (LANES - 1)
        row = x >> 7
        y = x
        at = nrow
        for o in range(1, 5):
            for a, b in halves[o]:
                for r in range(hrow):
                    line = got_send[o - 1, a, b : b + 1, r * LANES : (r + 1) * LANES]
                    line = jnp.broadcast_to(line + o * nrow * LANES, x.shape)
                    y = jnp.where(row == at, lane_gather(line, lane), y)
                    at += 1
        return y

    def compose_all():
        for o in order:
            arrived(rounds[1], o)
        for i in range(srows):
            for r in range(nrow):
                cols = slice(r * LANES, (r + 1) * LANES)
                y = compose(sq[i * 8 : i * 8 + 8, cols])
                sq[i * 8 : i * 8 + 8, cols] = y >> 7
                sl[i * 8 : i * 8 + 8, cols] = y & (LANES - 1)

    def compose_heads():
        for i in range(erow // 8):
            y = compose(head[i * 8 : i * 8 + 8, :])
            hq[i * 8 : i * 8 + 8, :] = y >> 7
            hl[i * 8 : i * 8 + 8, :] = y & (LANES - 1)

    srows = sq.shape[0] // 8

    def look(rnd, o, r, k, shape):
        at = o * vrow + k * nrow + r
        return jnp.broadcast_to(tab[rnd, at : at + 1, :], shape)

    def add_rows(rnd, o, rows, lanes, accs):
        for r in range(nrow):
            for i in range(len(rows)):
                hit = rows[i] == o * nrow + r
                for k in range(4):
                    v = lane_gather(look(rnd, o, r, k, rows[i].shape), lanes[i])
                    accs[i][k] = v if accs[i][k] is None else jnp.where(hit, v, accs[i][k])

    for rnd in range(SWEEPS):
        if rnd == 0:
            tab[rnd, :vrow, :] = bsc[...]
        copies = exchange(
            2 + rnd,
            lambda o: tab.at[rnd, pl.ds(0, vrow)],
            lambda o: tab.at[rnd, pl.ds(o * vrow, vrow)],
        )
        rounds.append(copies)
        if rnd == 0:
            compose_all()
        if rnd == 1:
            compose_heads()
        if rnd < SWEEPS - 1:
            where = [(slice(i * 8, i * 8 + 8), slice(r * LANES, (r + 1) * LANES)) for i in range(srows) for r in range(nrow)]
            rows = [sq[w] for w in where]
            lanes = [sl[w] for w in where]
            accs = [[None] * 4 for _ in where]
            add_rows(rnd, 0, rows, lanes, accs)
            for o in order:
                arrived(copies, o)
                add_rows(rnd, o, rows, lanes, accs)
            for k in range(4):
                for r in range(nrow):
                    total = None
                    for i in range(srows):
                        n = i * nrow + r
                        v = accs[n][k] * cf[(k,) + where[n]]
                        total = v if total is None else total + v
                    at = k * nrow + r
                    tab[rnd + 1, at : at + 1, :] = bsc[at : at + 1, :] - jnp.sum(total, axis=0, keepdims=True)

    last = SWEEPS - 1
    n3 = erow // 8
    where = [slice(i * 8, i * 8 + 8) for i in range(n3)]
    tails = [tail[w, :] for w in where]
    tacc = [[None] * 4 for _ in where]
    add_rows(last, 0, [t >> 7 for t in tails], [t & (LANES - 1) for t in tails], tacc)
    rows = [hq[w, :] for w in where]
    lanes = [hl[w, :] for w in where]
    hacc = [[None] * 4 for _ in where]
    add_rows(last, 0, rows, lanes, hacc)
    for o in order:
        arrived(copies, o)
        add_rows(last, o, rows, lanes, hacc)
    for i, w in enumerate(where):
        mixed = None
        for c in range(3):
            v = tan2[c * erow + i * 8 : c * erow + i * 8 + 8, :] * (tacc[i][c + 1] + hacc[i][c + 1])
            mixed = v if mixed is None else mixed + v
        out_ref[w, :] = (hacc[i][0] - tacc[i][0]) + 0.5 * mixed

    for copies in rounds:
        for o in order:
            copies[o].wait_send()


def body(
    residual, edge_scale, tangent, edge_tail, edge_head,
    stencil_index, stencil_coef, diag_margin, send_index,
):
    edges = residual.shape[0]
    erow = edges // LANES
    nodes = diag_margin.shape[1]
    nrow = nodes // LANES
    vrow = 4 * nrow
    stencil = stencil_index.shape[0]
    spad = -(-stencil // 8) * 8
    hrow = send_index.shape[2] // LANES
    blocks = (nrow + 8 * hrow) // nrow
    coef = jnp.transpose(stencil_coef, (1, 0, 2))
    square = lambda x: x.reshape(erow, LANES)
    anyspace = pl.BlockSpec(memory_space=pl.ANY)
    vm = pltpu.VMEM
    i32 = jnp.int32
    gathered = pl.pallas_call(
        kernel,
        out_shape=jax.ShapeDtypeStruct((erow, LANES), F32),
        in_specs=[anyspace] * 8,
        out_specs=pl.BlockSpec(memory_space=vm),
        scratch_shapes=[
            vm((erow, LANES), F32),
            vm(tangent.shape, F32),
            vm((erow, LANES), i32),
            vm((erow, LANES), i32),
            vm(stencil_index.shape, i32),
            vm(coef.shape, BF16),
            vm(diag_margin.shape, F32),
            vm(send_index.shape, i32),
            vm((4,) + send_index.shape, i32),
            vm((32 * hrow, LANES), F32),
            vm((32 * hrow, LANES), F32),
            vm((SWEEPS, 5 * vrow, LANES), F32),
            vm((LANES, edges), BF16),
            vm((2 * vrow, edges), BF16),
            vm((LANES, edges), BF16),
            vm((2 * blocks * vrow, edges), BF16),
            vm((LANES, 4 * send_index.shape[2]), BF16),
            vm((2 * vrow, 4 * send_index.shape[2]), BF16),
            vm((16 * hrow, LANES), F32),
            vm((4, spad, nodes), F32),
            vm((vrow, LANES), F32),
            vm((vrow, LANES), F32),
            vm((erow, LANES), i32),
            vm((erow, LANES), i32),
            vm((spad, nodes), i32),
            vm((spad, nodes), i32),
            vm((3 * erow, LANES), F32),
            pltpu.SemaphoreType.DMA((8,)),
            pltpu.SemaphoreType.DMA((SWEEPS + 2, 4)),
            pltpu.SemaphoreType.DMA((SWEEPS + 2, 4)),
        ],
        compiler_params=pltpu.CompilerParams(collective_id=0, has_side_effects=True),
    )(
        square(residual), tangent, square(edge_tail), square(edge_head),
        stencil_index, coef, diag_margin, send_index,
    )
    return edge_scale * residual + gathered.reshape(edges)


def solution(mesh):
    return jax.shard_map(
        body,
        mesh=mesh,
        in_specs=(
            P(("grp", "sub")),
            P(("grp", "sub")),
            P(None, ("grp", "sub")),
            P(("grp", "sub")),
            P(("grp", "sub")),
            P(None, ("grp", "sub")),
            P(None, None, ("grp", "sub")),
            P(None, ("grp", "sub")),
            P("grp", "sub", None),
        ),
        out_specs=P(("grp", "sub")),
        check_vma=False,
    )
```

```python
import functools

import jax
import jax.numpy as jnp
from jax import lax
from jax.experimental import pallas as pl
from jax.experimental.pallas import tpu as pltpu
from jax.sharding import PartitionSpec as P

SWEEPS = 4
LANES = 128
OPP = (0, 2, 1, 4, 3)
MESH = pl.DeviceIdType.MESH
DNUMS = lax.GatherDimensionNumbers(
    offset_dims=(),
    collapsed_slice_dims=(1,),
    start_index_map=(1,),
    operand_batching_dims=(0,),
    start_indices_batching_dims=(0,),
)
F32 = jnp.float32
BF16 = jnp.bfloat16


def lane_gather(table, lane):
    return lax.gather(
        table,
        lane[..., None],
        DNUMS,
        slice_sizes=(1, 1),
        mode=lax.GatherScatterMode.PROMISE_IN_BOUNDS,
    )


def nt_dot(a, b):
    return lax.dot_general(a, b, (((1,), (1,)), ((), ())), preferred_element_type=F32)


def kernel(
    res_h, tan_h, tail_h, head_h, sidx_h, coef_h, marg_h, send_h,
    out_ref,
    res, tan, tail, head, sidx, coef, marg, own_send,
    got_send, psend, got_p, tab, onehot, spread, onehot2, spread2, onehot3, spread3, tsum,
    cf, bsc, diag, hq, hl, sq, sl, tan2,
    local_sem, send_sem, recv_sem,
):
    G, S = lax.axis_size("grp"), lax.axis_size("sub")
    g, s = lax.axis_index("grp"), lax.axis_index("sub")
    gm, gp = lax.rem(g + G - 1, G), lax.rem(g + 1, G)
    sm, sp = lax.rem(s + S - 1, S), lax.rem(s + 1, S)
    peer = (None, (gm, s), (gp, s), (g, sm), (g, sp))
    order = (4, 3, 2, 1)
    nrow = marg.shape[1] // LANES
    erow = res.shape[0]
    stencil = sidx.shape[0]
    vrow = 4 * nrow
    nq = 5 * nrow
    hrow = got_send.shape[3] // LANES

    barrier = pltpu.get_barrier_semaphore()
    for o in order:
        pl.semaphore_signal(barrier, inc=1, device_id=peer[o], device_id_type=MESH)
    pairs = (
        (tail_h, tail), (res_h, res), (tan_h, tan), (head_h, head),
        (send_h, own_send), (coef_h, coef), (marg_h, marg), (sidx_h, sidx),
    )
    local = [
        pltpu.make_async_copy(src, dst, local_sem.at[i]) for i, (src, dst) in enumerate(pairs)
    ]
    for c in local:
        c.start()

    def exchange(rnd, src, dst):
        copies = {}
        for o in order:
            copies[o] = pltpu.make_async_remote_copy(
                src_ref=src(o),
                dst_ref=dst(OPP[o]),
                send_sem=send_sem.at[rnd, o - 1],
                recv_sem=recv_sem.at[rnd, OPP[o] - 1],
                device_id=peer[o],
                device_id_type=MESH,
            )
            copies[o].start()
        return copies

    def arrived(copies, o):
        copies[OPP[o]].wait_recv()

    near = 2 - lax.rem(g, 2)
    walk = (4, 3, near, 3 - near)

    def table_here(rnd, o):
        pltpu.make_async_remote_copy(
            src_ref=tab.at[rnd, pl.ds(0, vrow)],
            dst_ref=tab.at[rnd, pl.ds(o * vrow, vrow)],
            send_sem=send_sem.at[2 + rnd, 0],
            recv_sem=recv_sem.at[2 + rnd, o - 1],
            device_id=peer[4],
            device_id_type=MESH,
        ).wait_recv()

    for c in local:
        c.wait()
    riota = lax.broadcasted_iota(jnp.int32, (vrow, LANES), 0)
    kind = riota // nrow
    rpart = riota - kind * nrow
    liota = lax.broadcasted_iota(jnp.int32, (LANES, LANES), 0)

    def terms(t, sign):
        r = res[t : t + 1, :]
        first = jnp.broadcast_to(r if sign > 0 else -r, (vrow, LANES))
        half = 0.5 * r
        val = first
        for c in range(3):
            v = tan[c : c + 1, t * LANES : (t + 1) * LANES] * half
            val = jnp.where(kind == c + 1, v, val)
        hi = val.astype(BF16).astype(F32)
        return hi, val - hi

    def scatter(spread_ref, onehot_ref, lanes_of, rows_of, owners, sign):
        for t in range(erow):
            cols = slice(t * LANES, (t + 1) * LANES)
            onehot_ref[:, cols] = jnp.where(liota == lanes_of(t), 1.0, 0.0).astype(BF16)
            hi, lo = terms(t, sign)
            row = rows_of(t)
            for o in range(owners):
                hit = row == rpart + o * nrow
                for p, v in enumerate((hi, lo)):
                    base = (p * owners + o) * vrow
                    spread_ref[base : base + vrow, cols] = jnp.where(hit, v, 0.0).astype(BF16)
        both = nt_dot(spread_ref[...], onehot_ref[...])
        return both[: owners * vrow] + both[owners * vrow :]

    own_sum = scatter(
        spread, onehot,
        lambda t: tail[t : t + 1, :] & (LANES - 1),
        lambda t: tail[t : t + 1, :] >> 7,
        1, -1,
    )

    parts = scatter(
        spread2, onehot2,
        lambda t: head[t : t + 1, :] & (LANES - 1),
        lambda t: head[t : t + 1, :] >> 7,
        (nrow + 8 * hrow) // nrow, 1,
    )
    psend[...] = parts[vrow:]
    own_sum = own_sum + parts[:vrow]
    sent = 2 * 4 * hrow

    lists = tuple((a, b, r) for a in range(2) for b in range(2) for r in range(hrow))

    def own_list(a, b, r):
        return own_send[a, b : b + 1, r * LANES : (r + 1) * LANES]

    for n, abr in enumerate(lists):
        hit = liota == (own_list(*abr) & (LANES - 1))
        onehot3[:, n * LANES : (n + 1) * LANES] = jnp.where(hit, 1.0, 0.0).astype(BF16)

    cf[...] = jnp.zeros_like(cf)
    for k in range(4):
        for r in range(nrow):
            cols = slice(r * LANES, (r + 1) * LANES)
            c = coef[:, k, cols].astype(F32)
            d = (1.0 + marg[k : k + 1, cols]) * jnp.sum(jnp.abs(c), axis=0, keepdims=True)
            inv = 1.0 / d
            diag[k * nrow + r : k * nrow + r + 1, :] = inv
            cf[k, :stencil, cols] = c * inv
    for c in range(3):
        for t in range(erow):
            tan2[c * erow + t : c * erow + t + 1, :] = tan[c : c + 1, t * LANES : (t + 1) * LANES]
    sq[...] = jnp.zeros_like(sq)
    sq[:stencil, :] = sidx[...]

    pl.semaphore_wait(barrier, 4)
    rounds = [
        exchange(
            1,
            lambda o: psend.at[pl.ds((o - 1) * sent, sent)],
            lambda o: got_p.at[pl.ds((o - 1) * sent, sent)],
        )
    ]
    rounds.append(exchange(0, lambda o: own_send, lambda o: got_send.at[o - 1]))

    for o in order:
        arrived(rounds[0], o)
    block = 4 * hrow
    for a in range(2):
        for b in range(2):
            first = a * sent + b * block
            second = (2 + b) * sent + a * block
            at = (a * 2 + b) * block
            tsum[at : at + block, :] = got_p[first : first + block, :] + got_p[second : second + block, :]
    for n, (a, b, r) in enumerate(lists):
        base = (a * 2 + b) * block + r
        val = jnp.broadcast_to(tsum[base : base + 1, :], (vrow, LANES))
        for k in range(1, 4):
            at = base + k * hrow
            val = jnp.where(kind == k, tsum[at : at + 1, :], val)
        hit = (own_list(a, b, r) >> 7) == rpart
        val = jnp.where(hit, val, 0.0)
        hi = val.astype(BF16)
        cols = slice(n * LANES, (n + 1) * LANES)
        spread3[:vrow, cols] = hi
        spread3[vrow:, cols] = (val - hi.astype(F32)).astype(BF16)
    back = nt_dot(spread3[...], onehot3[...])
    own_sum = own_sum + (back[:vrow] + back[vrow:])
    bsc[...] = own_sum * diag[...]

    halves = (
        None,
        ((1, 0), (1, 1)),
        ((0, 0), (0, 1)),
        ((0, 1), (1, 1)),
        ((0, 0), (1, 0)),
    )

    def compose(x):
        lane = x & (LANES - 1)
        row = x >> 7
        y = x
        at = nrow
        for o in range(1, 5):
            for a, b in halves[o]:
                for r in range(hrow):
                    line = got_send[o - 1, a, b : b + 1, r * LANES : (r + 1) * LANES]
                    line = jnp.broadcast_to(line + o * nrow * LANES, x.shape)
                    y = jnp.where(row == at, lane_gather(line, lane), y)
                    at += 1
        return y

    def compose_all():
        for o in order:
            arrived(rounds[1], o)
        for i in range(srows):
            for r in range(nrow):
                cols = slice(r * LANES, (r + 1) * LANES)
                y = compose(sq[i * 8 : i * 8 + 8, cols])
                sq[i * 8 : i * 8 + 8, cols] = y >> 7
                sl[i * 8 : i * 8 + 8, cols] = y & (LANES - 1)

    def compose_heads():
        for i in range(erow // 8):
            y = compose(head[i * 8 : i * 8 + 8, :])
            hq[i * 8 : i * 8 + 8, :] = y >> 7
            hl[i * 8 : i * 8 + 8, :] = y & (LANES - 1)

    srows = sq.shape[0] // 8

    def look(rnd, o, r, k, shape):
        at = o * vrow + k * nrow + r
        return jnp.broadcast_to(tab[rnd, pl.ds(at, 1), :], shape)

    def add_rows(rnd, o, rows, lanes, accs):
        for r in range(nrow):
            for i in range(len(rows)):
                hit = rows[i] == o * nrow + r
                for k in range(4):
                    v = lane_gather(look(rnd, o, r, k, rows[i].shape), lanes[i])
                    accs[i][k] = v if accs[i][k] is None else jnp.where(hit, v, accs[i][k])

    sub8 = lax.broadcasted_iota(jnp.int32, (8, LANES), 0)

    def fold(vecs):
        step = len(vecs) // 2
        while step:
            keep = (sub8 & step) == 0
            vecs = [
                jnp.where(keep, x, y) + pltpu.roll(jnp.where(keep, y, x), step, axis=0)
                if step == 4 else
                jnp.where(keep, x + pltpu.roll(x, 8 - step, axis=0), y + pltpu.roll(y, step, axis=0))
                for x, y in zip(vecs[:step], vecs[step:])
            ]
            step //= 2
        return vecs[0]

    for rnd in range(SWEEPS):
        if rnd == 0:
            tab[rnd, :vrow, :] = bsc[...]
        copies = exchange(
            2 + rnd,
            lambda o: tab.at[rnd, pl.ds(0, vrow)],
            lambda o: tab.at[rnd, pl.ds(o * vrow, vrow)],
        )
        rounds.append(copies)
        if rnd == 0:
            compose_all()
        if rnd == 1:
            compose_heads()
        if rnd < SWEEPS - 1:
            where = [(slice(i * 8, i * 8 + 8), slice(r * LANES, (r + 1) * LANES)) for i in range(srows) for r in range(nrow)]
            rows = [sq[w] for w in where]
            lanes = [sl[w] for w in where]
            accs = [[None] * 4 for _ in where]
            add_rows(rnd, 0, rows, lanes, accs)
            for o in walk:
                table_here(rnd, o)
                add_rows(rnd, o, rows, lanes, accs)
            totals = []
            for k in range(4):
                for r in range(nrow):
                    total = None
                    for i in range(srows):
                        n = i * nrow + r
                        v = accs[n][k] * cf[(k,) + where[n]]
                        total = v if total is None else total + v
                    totals.append(total)
            for at in range(0, vrow, 8):
                tab[rnd + 1, at : at + 8, :] = bsc[at : at + 8, :] - fold(totals[at : at + 8])

    last = SWEEPS - 1
    n3 = erow // 8
    where = [slice(i * 8, i * 8 + 8) for i in range(n3)]
    tails = [tail[w, :] for w in where]
    tacc = [[None] * 4 for _ in where]
    add_rows(last, 0, [t >> 7 for t in tails], [t & (LANES - 1) for t in tails], tacc)
    rows = [hq[w, :] for w in where]
    lanes = [hl[w, :] for w in where]
    hacc = [[None] * 4 for _ in where]
    add_rows(last, 0, rows, lanes, hacc)
    for o in walk:
        table_here(last, o)
        add_rows(last, o, rows, lanes, hacc)
    for i, w in enumerate(where):
        mixed = None
        for c in range(3):
            v = tan2[c * erow + i * 8 : c * erow + i * 8 + 8, :] * (tacc[i][c + 1] + hacc[i][c + 1])
            mixed = v if mixed is None else mixed + v
        out_ref[w, :] = (hacc[i][0] - tacc[i][0]) + 0.5 * mixed

    for copies in rounds:
        for o in order:
            copies[o].wait_send()


def body(
    residual, edge_scale, tangent, edge_tail, edge_head,
    stencil_index, stencil_coef, diag_margin, send_index,
):
    edges = residual.shape[0]
    erow = edges // LANES
    nodes = diag_margin.shape[1]
    nrow = nodes // LANES
    vrow = 4 * nrow
    stencil = stencil_index.shape[0]
    spad = -(-stencil // 8) * 8
    hrow = send_index.shape[2] // LANES
    blocks = (nrow + 8 * hrow) // nrow
    coef = jnp.transpose(stencil_coef, (1, 0, 2))
    square = lambda x: x.reshape(erow, LANES)
    anyspace = pl.BlockSpec(memory_space=pl.ANY)
    vm = pltpu.VMEM
    i32 = jnp.int32
    gathered = pl.pallas_call(
        kernel,
        out_shape=jax.ShapeDtypeStruct((erow, LANES), F32),
        in_specs=[anyspace] * 8,
        out_specs=pl.BlockSpec(memory_space=vm),
        scratch_shapes=[
            vm((erow, LANES), F32),
            vm(tangent.shape, F32),
            vm((erow, LANES), i32),
            vm((erow, LANES), i32),
            vm(stencil_index.shape, i32),
            vm(coef.shape, BF16),
            vm(diag_margin.shape, F32),
            vm(send_index.shape, i32),
            vm((4,) + send_index.shape, i32),
            vm((32 * hrow, LANES), F32),
            vm((32 * hrow, LANES), F32),
            vm((SWEEPS, 5 * vrow, LANES), F32),
            vm((LANES, edges), BF16),
            vm((2 * vrow, edges), BF16),
            vm((LANES, edges), BF16),
            vm((2 * blocks * vrow, edges), BF16),
            vm((LANES, 4 * send_index.shape[2]), BF16),
            vm((2 * vrow, 4 * send_index.shape[2]), BF16),
            vm((16 * hrow, LANES), F32),
            vm((4, spad, nodes), F32),
            vm((vrow, LANES), F32),
            vm((vrow, LANES), F32),
            vm((erow, LANES), i32),
            vm((erow, LANES), i32),
            vm((spad, nodes), i32),
            vm((spad, nodes), i32),
            vm((3 * erow, LANES), F32),
            pltpu.SemaphoreType.DMA((8,)),
            pltpu.SemaphoreType.DMA((SWEEPS + 2, 4)),
            pltpu.SemaphoreType.DMA((SWEEPS + 2, 4)),
        ],
        compiler_params=pltpu.CompilerParams(collective_id=0, has_side_effects=True),
    )(
        square(residual), tangent, square(edge_tail), square(edge_head),
        stencil_index, coef, diag_margin, send_index,
    )
    return edge_scale * residual + gathered.reshape(edges)


def solution(mesh):
    return jax.shard_map(
        body,
        mesh=mesh,
        in_specs=(
            P(("grp", "sub")),
            P(("grp", "sub")),
            P(None, ("grp", "sub")),
            P(("grp", "sub")),
            P(("grp", "sub")),
            P(None, ("grp", "sub")),
            P(None, None, ("grp", "sub")),
            P(None, ("grp", "sub")),
            P("grp", "sub", None),
        ),
        out_specs=P(("grp", "sub")),
        check_vma=False,
    )
```
